32 devices in a mesh: gx: 8 (over z, y), gy: 4 (over x, core).
Axes of the slice: x: 2, y: 2, z: 4, core: 2. Of those that a mesh axis runs over, the one named last changes fastest.
Arguments:
- scalar: float32 [2, 512, 8, 4, 128], P(None, None, 'gx', 'gy'), may hold values from -6 to 6
- velocity: float32 [3, 2, 512, 8, 4, 128], P(None, None, None, 'gx', 'gy'), may hold values from -1 to 1
- diffusivity: float32 [2, 8, 4, 128], P(None, 'gx', 'gy'), may hold values from 0.005 to 0.05
- recv_owner: int32 [65536, 1], P(('gx', 'gy')), may hold values from 0 to 31; in each aligned block of 2048 rows (0 to 2047, 2048 to 4095, ...) at most 128 rows name the same one
- donor_elem: int32 [65536], P(('gx', 'gy')), may hold values from 0 to 127
- recv_point: int32 [65536], P(('gx', 'gy')), may hold values from 0 to 65535
- recv_coords: float32 [3, 65536], P(None, ('gx', 'gy')), may hold values from -1 to 1
Outputs:
- advanced: float32 [2, 512, 8, 4, 128], P(None, None, 'gx', 'gy')
The draws below stay inside these ranges and needn't reach their ends.
Inputs may be any that keep to these rules, and one draw needn't show every extreme that they name: `recv_owner`: among the 2048 receivers of one device no owner is named more than 128 times, a bound that some block reaches.
All inputs are finite; a program needn't handle non-finite values.
Results may differ from the reference program's by a relative error of at most 0.0003.
Values sent between devices are 32-bit elements; how exact they have to be, the bound alone decides.
A program may use at most 128 MiB of HBM per device.

```python
import math
import jax
import jax.numpy as jnp
import numpy as np
from jax import lax

KX = 1
KY = 1
EZ = 128
R_DEV = 2048
ELEMS = 128
CAP = 128
EX = 8
EY = 4
RECV = 65536
N_GY = 4
DEVICES = 32


def set_ends(entries, own_key, smallest, largest):
    spot = [jax.random.randint(jax.random.fold_in(own_key, axis), (), 0, length) for axis, length in enumerate(entries.shape)]
    main_axis = entries.shape.index(max(entries.shape))
    next_to = spot[:main_axis] + [(spot[main_axis] + 1) % entries.shape[main_axis]] + spot[main_axis + 1:]
    return entries.at[tuple(spot)].set(smallest).at[tuple(next_to)].set(largest)


def block_levels(own_key, extent, shards, smallest, top_value):
    def one(dim, parts):
        heights = jax.random.uniform(jax.random.fold_in(jax.random.fold_in(own_key, 6), dim), (parts,), jnp.float32, smallest / len(shards), top_value / len(shards))
        return jnp.repeat(jnp.exp(heights), extent[dim] // parts).reshape((-1,) + (1,) * (len(extent) - dim - 1))

    factor_of = one(*shards[0])
    for cut in shards[1:]:
        factor_of = factor_of * one(*cut)
    return factor_of


def routed_block(key, own, number, rows, amount, top, most, skew):
    order = jax.random.permutation(key, amount)
    crowded, usual = load_shares(amount, rows * top, most, skew, True), load_shares(amount, rows * top, most, skew, False)
    places = jnp.arange(amount)

    def named(sizes, offset_by):
        used = int((sizes > 0).sum())
        fixed = max(1, used // 4)
        passed = fixed + (places - fixed + offset_by * (used - fixed)) % max(1, amount - fixed)
        return jnp.zeros((amount,), jnp.int32).at[order[jnp.where(places < fixed, places, passed)]].set(jnp.asarray(sizes, jnp.int32))

    sizes = jnp.where(number % 4 == 0, named(crowded, number // 4), named(usual, number - number // 4 - 1))
    mixed = jax.random.permutation(jax.random.fold_in(own, 3), amount)
    source_of, sink = mixed[0:amount // 2 * 2:2], mixed[1:amount // 2 * 2:2]
    slack = jnp.minimum(sizes[source_of] - 1, most - sizes[sink]) // 2
    slack = jnp.where((source_of == order[0]) | (sink == order[0]) | (sizes[sink] == 0), 0, jnp.maximum(slack, 0))
    passed = jax.random.randint(jax.random.fold_in(own, 4), (amount // 2,), 0, 1 << 20) % (slack + 1)
    sizes = sizes.at[source_of].add(-passed).at[sink].add(passed)
    members = jnp.searchsorted(jnp.cumsum(sizes), jnp.arange(rows * top), side="right").astype(jnp.int32)
    grid = members.reshape(top, rows).T
    grid = grid[jax.random.permutation(jax.random.fold_in(own, 1), rows)]
    offset_by = jax.random.randint(jax.random.fold_in(own, 2), (rows, 1), 0, top)
    return jnp.take_along_axis(grid, (jnp.arange(top)[None, :] + offset_by) % top, axis=1)


def load_shares(number_of, total, reach, lean, full):
    portions = [(1 << 20) // math.isqrt(grade ** lean) + 1 for grade in range(1, number_of + 1)]
    largest = reach if full else min(reach, max(-(-total // number_of), total * portions[0] // sum(portions)))
    least = 1 if total - largest >= number_of - 1 else 0
    holding, rest = [largest] + [least] * (number_of - 1), total - largest - least * (number_of - 1)
    while rest > 0:
        movable = [i for i in range(1, number_of) if holding[i] < largest] or [i for i in range(1, number_of) if holding[i] < reach]
        pool, remaining = sum([portions[i] for i in movable]), rest
        for i in movable:
            addition = min(reach - holding[i], max(1, remaining * portions[i] // pool), rest)
            holding[i] = holding[i] + addition
            rest = rest - addition
    return np.array(holding)


def bell_draw(rng, extent, scale, bound, shards=(), kind=jnp.bfloat16):
    loudness = block_levels(rng, extent, shards, -0.22, 0.18) if shards else 1.0
    result = jax.random.normal(rng, extent, jnp.float32) * scale * loudness
    return jnp.minimum(jnp.maximum(result, -bound), bound).astype(kind)


def setup_inputs(seed: int = 0) -> dict:
    streams_of = jax.random.split(jax.random.key(seed), 8)
    scalar = bell_draw(streams_of[0], (2, 512, EX, EY, EZ), 1.0, 6.0, ((2, 8), (3, 4)), jnp.float32)
    velocity = jnp.clip(jax.random.uniform(streams_of[1], (3, 2, 512, EX, EY, EZ), jnp.float32, -1.0, 1.0) * block_levels(streams_of[1], (3, 2, 512, EX, EY, EZ), ((3, 8), (4, 4)), -0.4, 0.0), -1.0, 1.0)
    diffusivity = jnp.clip(jnp.exp(math.log(0.05) - 2.3025851 * jax.random.uniform(streams_of[2], (2, EX, EY, EZ), jnp.float32) ** block_levels(streams_of[2], (2, EX, EY, EZ), ((1, 8), (2, 4)), -0.2, 0.2)), 0.005, 0.05)
    recv_owner_keys = jax.random.split(jax.random.fold_in(streams_of[3], 1), RECV // R_DEV)
    recv_owner_turns = jax.random.permutation(jax.random.fold_in(streams_of[3], 3), RECV // R_DEV)
    recv_owner = jax.vmap(lambda own, number: routed_block(jax.random.fold_in(streams_of[3], 2), own, number, R_DEV, DEVICES, 1, CAP, 2))(recv_owner_keys, recv_owner_turns).reshape((RECV, 1))
    donor_elem = set_ends(jax.random.randint(streams_of[4], (RECV,), 0, ELEMS), jax.random.fold_in(streams_of[4], 1), 0, ELEMS - 1).astype(jnp.int32)
    recv_point = set_ends(jax.random.randint(streams_of[5], (RECV,), 0, 512 * ELEMS), jax.random.fold_in(streams_of[5], 1), 0, (512 * ELEMS) - 1).astype(jnp.int32)
    recv_coords = jnp.clip(jax.random.uniform(streams_of[6], (3, RECV), jnp.float32, -1.0, 1.0) * block_levels(streams_of[6], (3, RECV), ((1, 32),), -0.4, 0.0), -1.0, 1.0)
    return {"scalar": scalar, "velocity": velocity, "diffusivity": diffusivity, "recv_owner": recv_owner, "donor_elem": donor_elem, "recv_point": recv_point, "recv_coords": recv_coords}


time_step = 0.01
penalty_rate = 50.0
metric = 2.0
volume_factor = 0.125
node_inner = [0.871740148509606615337, 0.591700181433142302144, 0.209299217902478868769]


def legendre_seven(point):
    before, current = 1.0, point
    for order in range(1, 7):
        before, current = current, ((2 * order + 1) * point * current - order * before) / (order + 1)
    return current


def gll_tables():
    degree = 7
    gll_nodes = [-1.0, -node_inner[0], -node_inner[1], -node_inner[2], node_inner[2], node_inner[1], node_inner[0], 1.0]
    end_values = [legendre_seven(v) for v in gll_nodes]
    weights = [2.0 / (degree * (degree + 1) * v * v) for v in end_values]
    derivative = [[0.0] * 8 for _ in range(8)]
    for a in range(8):
        for b in range(8):
            if a != b:
                derivative[a][b] = end_values[a] / (end_values[b] * (gll_nodes[a] - gll_nodes[b]))
    derivative[0][0] = -degree * (degree + 1) / 4.0
    derivative[7][7] = degree * (degree + 1) / 4.0
    weight_row = jnp.asarray(weights, jnp.float32)
    cube_weights = weight_row[:, None, None] * weight_row[None, :, None] * weight_row[None, None, :]
    return gll_nodes, cube_weights, derivative


def lagrange_rows(position, gll_nodes):
    columns = []
    for j in range(8):
        factor = jnp.ones_like(position)
        for m in range(8):
            if m != j:
                factor = factor * ((position - gll_nodes[m]) / (gll_nodes[j] - gll_nodes[m]))
        columns.append(factor)
    return jnp.stack(columns, axis=-1)


def element_rate(values, velocity, diffusivity, derivative, cube_weights):
    highest = lax.Precision.HIGHEST
    grad_x = metric * jnp.einsum('ai,ijkxyz->ajkxyz', derivative, values, precision=highest)
    grad_y = metric * jnp.einsum('bj,ijkxyz->ibkxyz', derivative, values, precision=highest)
    grad_z = metric * jnp.einsum('ck,ijkxyz->ijcxyz', derivative, values, precision=highest)
    mass_local = volume_factor * cube_weights[:, :, :, None, None, None]
    advect = velocity[0] * grad_x + velocity[1] * grad_y + velocity[2] * grad_z
    scaled = (metric * mass_local) * diffusivity[None, None, None]
    diffuse = jnp.einsum('ai,ajkxyz->ijkxyz', derivative, scaled * grad_x, precision=highest)
    diffuse = diffuse + jnp.einsum('bj,ibkxyz->ijkxyz', derivative, scaled * grad_y, precision=highest)
    diffuse = diffuse + jnp.einsum('ck,ijcxyz->ijkxyz', derivative, scaled * grad_z, precision=highest)
    return -(mass_local * advect) - diffuse


def face_sum(values, pdim, edim, next_slab, prev_slab):
    left = lax.index_in_dim(values, 0, pdim, keepdims=True)
    right = lax.index_in_dim(values, 7, pdim, keepdims=True)
    count = values.shape[edim]
    after = jnp.concatenate([lax.slice_in_dim(left, 1, count, axis=edim), next_slab], axis=edim)
    before = jnp.concatenate([prev_slab, lax.slice_in_dim(right, 0, count - 1, axis=edim)], axis=edim)
    middle = lax.slice_in_dim(values, 1, 7, axis=pdim)
    return jnp.concatenate([left + before, middle, right + after], axis=pdim)


def assemble(values):
    for pdim, edim in ((1, 4), (2, 5), (3, 6)):
        slab = lax.index_in_dim(lax.index_in_dim(values, 0, pdim, keepdims=True), 0, edim, keepdims=True)
        zeros_slab = jnp.zeros_like(slab)
        values = face_sum(values, pdim, edim, zeros_slab, zeros_slab)
    return values


def reference(scalar, velocity, diffusivity, recv_owner, donor_elem, recv_point, recv_coords):
    gll_nodes, cube_np, derivative_np = gll_tables()
    derivative = jnp.asarray(derivative_np, jnp.float32)
    cube_weights = jnp.asarray(cube_np, jnp.float32)
    cube_flat = cube_weights.reshape(512)
    shape_full = (2, 8, 8, 8, EX, EY, EZ)
    elems = KX * KY * EZ
    flow = velocity.reshape((3,) + shape_full)
    mass_total = assemble(jnp.broadcast_to(volume_factor * cube_weights[None, :, :, :, None, None, None], shape_full))

    rows = jnp.arange(RECV, dtype=jnp.int32)
    device = rows // R_DEV
    local_row = rows % R_DEV
    dev_x = device // N_GY
    dev_y = device % N_GY
    own_mesh = (local_row >= R_DEV // 2).astype(jnp.int32)
    donor_mesh = 1 - own_mesh
    owners = recv_owner[:, 0]
    donor_x = (owners // N_GY) * KX + donor_elem // (KY * EZ)
    donor_y = (owners % N_GY) * KY + (donor_elem // EZ) % KY
    donor_z = donor_elem % EZ
    point_q = recv_point // elems
    point_e = recv_point % elems
    recv_x = dev_x * KX + point_e // (KY * EZ)
    recv_y = dev_y * KY + (point_e // EZ) % KY
    recv_z = point_e % EZ
    flat_index = ((own_mesh * 512 + point_q) * EX + recv_x) * (EY * EZ) + recv_y * EZ + recv_z
    basis_x = lagrange_rows(recv_coords[0], gll_nodes)
    basis_y = lagrange_rows(recv_coords[1], gll_nodes)
    basis_z = lagrange_rows(recv_coords[2], gll_nodes)
    point_mass = volume_factor * cube_flat[point_q]

    def blocks(array):
        return array.reshape((DEVICES, R_DEV) + array.shape[1:])

    def interpolate(values_five):
        def one_block(pieces):
            mesh_ids, elem_x, elem_y, elem_z, wx, wy, wz = pieces
            element_values = values_five[mesh_ids, :, elem_x, elem_y, elem_z]
            tensor_weights = (wx[:, :, None, None] * wy[:, None, :, None] * wz[:, None, None, :]).reshape(-1, 512)
            return jnp.sum(element_values * tensor_weights, axis=1)
        pieces = (blocks(donor_mesh), blocks(donor_x), blocks(donor_y), blocks(donor_z),
                  blocks(basis_x), blocks(basis_y), blocks(basis_z))
        return lax.map(one_block, pieces).reshape(RECV)

    def rate(values):
        local = jnp.stack([element_rate(values[m], flow[:, m], diffusivity[m], derivative, cube_weights) for m in range(2)])
        donor_values = interpolate(values.reshape(2, 512, EX, EY, EZ))
        current = values.reshape(-1)[flat_index]
        added = penalty_rate * point_mass * (donor_values - current)
        local = local.reshape(-1).at[flat_index].add(added).reshape(shape_full)
        return assemble(local) / mass_total

    start = scalar.reshape(shape_full)
    first = start + time_step * rate(start)
    second = 0.75 * start + 0.25 * (first + time_step * rate(first))
    third = start / 3.0 + (2.0 / 3.0) * (second + time_step * rate(second))
    return third.reshape(2, 512, EX, EY, EZ)
```

```python
import functools
import jax
import jax.numpy as jnp
import numpy as np
from jax import lax
from jax.experimental import pallas as pl
from jax.experimental.pallas import tpu as pltpu
from jax.sharding import PartitionSpec as P

time_step = 0.01
penalty_rate = 50.0
metric = 2.0
volume_factor = 0.125
node_inner = [0.8717401485096066, 0.5917001814331423, 0.20929921790247888]


def legendre_seven(point):
    before, current = (1.0, point)
    for order in range(1, 7):
        before, current = (
            current,
            ((2 * order + 1) * point * current - order * before) / (order + 1),
        )
    return current


def gll_tables():
    degree = 7
    gll_nodes = [
        -1.0,
        -node_inner[0],
        -node_inner[1],
        -node_inner[2],
        node_inner[2],
        node_inner[1],
        node_inner[0],
        1.0,
    ]
    end_values = [legendre_seven(v) for v in gll_nodes]
    weights = [2.0 / (degree * (degree + 1) * v * v) for v in end_values]
    derivative = [[0.0] * 8 for _ in range(8)]
    for a in range(8):
        for b in range(8):
            if a != b:
                derivative[a][b] = end_values[a] / (end_values[b] * (gll_nodes[a] - gll_nodes[b]))
    derivative[0][0] = -degree * (degree + 1) / 4.0
    derivative[7][7] = degree * (degree + 1) / 4.0
    weight_row = jnp.asarray(weights, jnp.float32)
    cube_weights = weight_row[:, None, None] * weight_row[None, :, None] * weight_row[None, None, :]
    return (gll_nodes, cube_weights, derivative)


def lagrange_rows(position, gll_nodes):
    columns = []
    for j in range(8):
        factor = jnp.ones_like(position)
        for m in range(8):
            if m != j:
                factor = factor * ((position - gll_nodes[m]) / (gll_nodes[j] - gll_nodes[m]))
        columns.append(factor)
    return jnp.stack(columns, axis=-1)


MESH = pl.DeviceIdType.MESH
HEADINGS = [(-1, 0), (1, 0), (0, -1), (0, 1), (-1, -1), (-1, 1), (1, -1), (1, 1)]


def halves(value):
    high = value.astype(jnp.bfloat16)
    return high, (value - high.astype(jnp.float32)).astype(jnp.bfloat16)


def mm(a, b):
    return jnp.dot(a, b, preferred_element_type=jnp.float32)


def mm_t(a, b):
    return lax.dot_general(a, b, (((1,), (1,)), ((), ())), preferred_element_type=jnp.float32)


def mm3(op_high, op_low, value):
    high, low = halves(value)
    return mm(op_high, high) + mm(op_high, low) + mm(op_low, high)


def step_kernel(
    derivative, start_ref, vel_ref, nu_ref, wm_ref, dim_ref, ops_ref, basis_ref, donor_ref, slot_q_ref, slot_e_ref,
    out_ref,
    cur, local, work, grad, pick, spread_q, spread_e, count, ans, rep, hx, hy, he,
    ans_send, ans_recv, halo_send, halo_recv,
):
    gx, gy = lax.axis_index("gx"), lax.axis_index("gy")
    nx, ny = lax.axis_size("gx"), lax.axis_size("gy")
    n = nx * ny
    me = gx * ny + gy
    ez = start_ref.shape[-1]
    groups, _, lanes = donor_ref.shape
    cap = ans.shape[-1]
    per = lanes // cap

    barrier = pltpu.get_barrier_semaphore()

    def greet(step, carry):
        d = lax.rem(me + step, n)
        pl.semaphore_signal(barrier, inc=1, device_id=(d // ny, lax.rem(d, ny)), device_id_type=MESH)
        return carry

    hx[...] = jnp.zeros_like(hx)
    hy[...] = jnp.zeros_like(hy)
    he[...] = jnp.zeros_like(he)
    lax.fori_loop(1, n, greet, 0)

    count[...] = jnp.zeros_like(count)

    def build(g, carry):
        wide = lax.broadcasted_iota(jnp.int32, (2 * ez, lanes), 0)
        tall = lax.broadcasted_iota(jnp.int32, (512, lanes), 0)
        pick[g] = jnp.where(wide == donor_ref[g], 1.0, 0.0).astype(jnp.bfloat16)
        spread_e[g] = jnp.where(wide == slot_e_ref[g], 1.0, 0.0).astype(jnp.bfloat16)
        spread_q[g] = jnp.where(tall == slot_q_ref[g], 1.0, 0.0).astype(jnp.bfloat16)
        count[...] += mm_t(spread_q[g], spread_e[g])
        return carry

    lax.fori_loop(0, groups, build, 0)
    cur[...] = start_ref[...]
    pl.semaphore_wait(barrier, n - 1)

    def halo_copy(s, number):
        dx, dy = HEADINGS[number]
        rows = pl.ds(0 if dy < 0 else 56, 8)
        plane = 0 if dx < 0 else 7
        if dy == 0:
            source, target = local.at[:, plane], hx.at[s, number]
        elif dx == 0:
            source, target = local.at[:, :, rows, :], hy.at[s, number - 2]
        else:
            source, target = local.at[:, plane, rows, :], he.at[s, number - 4]
        return pltpu.make_async_remote_copy(
            src_ref=source, dst_ref=target, send_sem=halo_send.at[s, number], recv_sem=halo_recv.at[s, number],
            device_id=(gx + dx, gy + dy), device_id_type=MESH,
        )

    def inside(dx, dy):
        return (gx + dx >= 0) & (gx + dx < nx) & (gy + dy >= 0) & (gy + dy < ny)

    for s in range(3):
        both = jnp.concatenate([cur[0].reshape(512, ez), cur[1].reshape(512, ez)], axis=1)
        high, low = halves(both)

        def interpolate(g, carry):
            found = mm(high, pick[g]) + mm(low, pick[g])
            acc = found[0:64] * basis_ref[g, 0:1, :]
            for i in range(1, 8):
                acc = acc + found[64 * i:64 * i + 64] * basis_ref[g, i:i + 1, :]
            acc2 = acc[0:8] * basis_ref[g, 8:9, :]
            for j in range(1, 8):
                acc2 = acc2 + acc[8 * j:8 * j + 8] * basis_ref[g, 8 + j:9 + j, :]
            row = jnp.sum(acc2 * basis_ref[g, 16:24, :], axis=0, keepdims=True)
            for t in range(per):
                ans[s, g * per + t] = row[:, t * cap:(t + 1) * cap]
            return carry

        lax.fori_loop(0, groups, interpolate, 0)

        def send(step, carry):
            d = lax.rem(me + step, n)
            pltpu.make_async_remote_copy(
                src_ref=ans.at[s, d], dst_ref=rep.at[s, me], send_sem=ans_send.at[s], recv_sem=ans_recv.at[s],
                device_id=(d // ny, lax.rem(d, ny)), device_id_type=MESH,
            ).start()
            return carry

        lax.fori_loop(1, n, send, 0)

        for m in range(2):
            lo_lane = m * ez
            scale = nu_ref[m:m + 1, :]
            for half in range(2):
                part = cur[m, 4 * half:4 * half + 4].reshape(256, ez)
                grad[0, 4 * half:4 * half + 4, :, lo_lane:lo_lane + ez] = mm3(ops_ref[0], ops_ref[1], part).reshape(4, 64, ez)
                grad[1, 4 * half:4 * half + 4, :, lo_lane:lo_lane + ez] = mm3(ops_ref[2], ops_ref[3], part).reshape(4, 64, ez)
            for a in range(8):
                gxa = (2.0 * derivative[a][0]) * cur[m, 0]
                for i in range(1, 8):
                    gxa = gxa + (2.0 * derivative[a][i]) * cur[m, i]
                wm = wm_ref[a]
                gya = grad[0, a, :, lo_lane:lo_lane + ez]
                gza = grad[1, a, :, lo_lane:lo_lane + ez]
                adv = vel_ref[0, m, a] * gxa + vel_ref[1, m, a] * gya + vel_ref[2, m, a] * gza
                local[m, a] = -(wm * adv)
                wn = wm * scale
                work[m, a] = wn * gxa
                grad[0, a, :, lo_lane:lo_lane + ez] = wn * gya
                grad[1, a, :, lo_lane:lo_lane + ez] = wn * gza
            for half in range(2):
                part_y = grad[0, 4 * half:4 * half + 4, :, lo_lane:lo_lane + ez].reshape(256, ez)
                part_z = grad[1, 4 * half:4 * half + 4, :, lo_lane:lo_lane + ez].reshape(256, ez)
                back = mm3(ops_ref[4], ops_ref[5], part_y) + mm3(ops_ref[6], ops_ref[7], part_z)
                local[m, 4 * half:4 * half + 4] -= back.reshape(4, 64, ez)
            for i in range(8):
                total = (2.0 * derivative[0][i]) * work[m, 0]
                for a in range(1, 8):
                    total = total + (2.0 * derivative[a][i]) * work[m, a]
                local[m, i] -= total

        rep[s, me] = ans[s, me]
        whole = rep.at[s, pl.ds(0, n - 1)]
        pltpu.make_async_copy(whole, whole, ans_recv.at[s]).wait()

        work[...] = jnp.zeros_like(work)

        def scatter(g, carry):
            row = jnp.concatenate([rep[s, g * per + t] for t in range(per)], axis=1)
            row_high, row_low = halves(row)
            where_e = spread_e[g]
            added = mm_t(spread_q[g], where_e * row_high) + mm_t(spread_q[g], where_e * row_low)
            work[0] += added[:, :ez].reshape(8, 64, ez)
            work[1] += added[:, ez:].reshape(8, 64, ez)
            return carry

        lax.fori_loop(0, groups, scatter, 0)
        for m in range(2):
            for i in range(8):
                held = count[64 * i:64 * i + 64, m * ez:(m + 1) * ez]
                local[m, i] += penalty_rate * wm_ref[i] * (work[m, i] - held * cur[m, i])

        for number, (dx, dy) in enumerate(HEADINGS):
            @pl.when(inside(dx, dy))
            def _(number=number):
                halo_copy(s, number).start()

        for number, (dx, dy) in enumerate(HEADINGS):
            @pl.when(inside(-dx, -dy))
            def _(number=number):
                halo_copy(s, number).wait_recv()

        work[...] = local[...]
        for m in range(2):
            work[m, 7] += hx[s, 0, m]
            work[m, 0] += hx[s, 1, m]
            work[m, :, 56:64, :] += hy[s, 0, m]
            work[m, :, 0:8, :] += hy[s, 1, m]
            work[m, 7, 56:64, :] += he[s, 0, m]
            work[m, 7, 0:8, :] += he[s, 1, m]
            work[m, 0, 56:64, :] += he[s, 2, m]
            work[m, 0, 0:8, :] += he[s, 3, m]

        for m in range(2):
            flat = work[m].reshape(512, ez)
            depth = lax.rem(lax.broadcasted_iota(jnp.int32, (512, ez), 0), 8)
            lane = lax.broadcasted_iota(jnp.int32, (512, ez), 1)
            after = pltpu.roll(pltpu.roll(flat, 7, 0), ez - 1, 1)
            before = pltpu.roll(pltpu.roll(flat, 505, 0), 1, 1)
            flat = flat + jnp.where((depth == 7) & (lane < ez - 1), after, 0.0)
            flat = flat + jnp.where((depth == 0) & (lane > 0), before, 0.0)
            moved = cur[m] + flat.reshape(8, 64, ez) * dim_ref[...]
            if s == 0:
                cur[m] = moved
            elif s == 1:
                cur[m] = 0.75 * start_ref[m] + 0.25 * moved
            else:
                out_ref[m] = start_ref[m] / 3.0 + 2.0 / 3.0 * moved

        for number, (dx, dy) in enumerate(HEADINGS):
            @pl.when(inside(dx, dy))
            def _(number=number):
                halo_copy(s, number).wait_send()

    for s in range(3):
        whole = ans.at[s, pl.ds(0, n - 1)]
        pltpu.make_async_copy(whole, whole, ans_send.at[s]).wait()


def split_host(matrix):
    high = matrix.astype(jnp.bfloat16)
    low = (matrix - high.astype(np.float64)).astype(jnp.bfloat16)
    return [high, low]


def body(scalar, velocity, diffusivity, recv_owner, donor_elem, recv_point, recv_coords):
    gll_nodes, cube_weights, derivative = gll_tables()
    ez = scalar.shape[4]
    elems = scalar.shape[2] * scalar.shape[3] * ez
    width_x, width_y = lax.axis_size("gx"), lax.axis_size("gy")
    n = width_x * width_y
    rows = recv_owner.shape[0]
    cap = max(2, 2 * rows // n)
    slots_all = n * cap
    per = max(1, min(n, 512 // cap))
    groups, lanes = n // per, per * cap

    owners = recv_owner[:, 0]
    bf, f32 = jnp.bfloat16, jnp.float32
    hot = (owners[None, :] == jnp.arange(n, dtype=jnp.int32)[:, None]).astype(bf)
    width = min(256, rows)
    blocks = rows // width
    earlier = jnp.asarray(np.triu(np.ones((width, width)), 1), bf)
    hot3 = hot.reshape(n, blocks, width)
    within = jnp.einsum("nbr,rs->nbs", hot3, earlier, preferred_element_type=f32)
    sums = jnp.sum(hot3.astype(f32), axis=2)
    strict = np.triu(np.ones((blocks, blocks)), 1).astype(np.float32)
    offset = jnp.sum(sums[:, :, None] * strict[None], axis=1)
    rank = jnp.sum((within + offset[:, :, None]) * hot3.astype(f32), axis=0).reshape(rows)
    slot_hot = (rank[None, :].astype(jnp.int32) == jnp.arange(cap, dtype=jnp.int32)[:, None]).astype(bf)

    own_mesh = (jnp.arange(rows, dtype=jnp.int32) >= rows // 2).astype(jnp.int32)
    point_q, point_e = recv_point // elems, recv_point % elems
    high = lax.reduce_precision(recv_coords, 8, 7)
    middle = lax.reduce_precision(recv_coords - high, 8, 7)
    low = recv_coords - high - middle
    ints = jnp.stack([donor_elem, 1 - own_mesh, point_q // 8 + 1, point_q % 8, point_e, own_mesh]).astype(f32)
    data = jnp.concatenate([high, middle, low, ints], axis=0).astype(bf)
    routed = jnp.einsum("cnr,kr->nck", data[:, None, :] * hot[None], slot_hot, preferred_element_type=f32)
    coords = routed[:, 0:3] + routed[:, 3:6] + routed[:, 6:9]
    asked = jnp.concatenate([coords, routed[:, 9:10] + elems * routed[:, 10:11]], axis=1)
    received = lax.all_to_all(asked, ("gx", "gy"), split_axis=0, concat_axis=0, tiled=True)
    received = jnp.moveaxis(received.reshape(groups, per, 4, cap), 2, 1).reshape(groups, 4, lanes)

    def grouped(piece):
        return piece.astype(jnp.int32).reshape(groups, 1, lanes)

    slot_q = grouped((routed[:, 11] - 1.0) * 8.0 + routed[:, 12])
    slot_e = grouped(routed[:, 13] + elems * routed[:, 14])
    donor = received[:, 3:4].astype(jnp.int32)
    basis = jnp.moveaxis(lagrange_rows(received[:, 0:3], gll_nodes), 3, 2).reshape(groups, 24, lanes)

    half_eye = np.eye(4)
    table = 2.0 * np.asarray(derivative, np.float64)
    along_y = np.kron(half_eye, np.kron(table, np.eye(8)))
    along_z = np.kron(half_eye, np.kron(np.eye(8), table))
    ops = []
    for matrix in (along_y, along_z, along_y.T, along_z.T):
        ops = ops + split_host(matrix)
    ops = jnp.asarray(np.stack(ops))

    weights = np.asarray([2.0 / (56.0 * legendre_seven(v) ** 2) for v in gll_nodes], np.float64)
    shared = jnp.asarray(weights + weights[::-1] * (np.arange(8) % 7 == 0), f32)
    single = jnp.asarray(weights, f32)
    ends = jnp.arange(8)

    def line_mass(position, count):
        joined = ((ends == 0) & (position > 0)) | ((ends == 7) & (position < count - 1))
        return jnp.where(joined, shared, single)

    mass_x = line_mass(lax.axis_index("gx"), width_x)
    mass_y = line_mass(lax.axis_index("gy"), width_y)
    place = jnp.arange(ez)[None, :]
    joined_z = ((ends[:, None] == 0) & (place > 0)) | ((ends[:, None] == 7) & (place < ez - 1))
    mass_z = jnp.where(joined_z, shared[:, None], single[:, None])
    mass = volume_factor * mass_x[:, None, None, None] * mass_y[None, :, None, None] * mass_z[None, None]
    step_mass = (time_step / mass).reshape(8, 64, ez)
    wm = jnp.broadcast_to((volume_factor * cube_weights).reshape(8, 64, 1), (8, 64, ez))

    vmem = pltpu.VMEM
    out = pl.pallas_call(
        functools.partial(step_kernel, derivative),
        out_shape=jax.ShapeDtypeStruct((2, 8, 64, ez), f32),
        in_specs=[pl.BlockSpec(memory_space=vmem)] * 10,
        out_specs=pl.BlockSpec(memory_space=vmem),
        scratch_shapes=[
            vmem((2, 8, 64, ez), f32),
            vmem((2, 8, 64, ez), f32),
            vmem((2, 8, 64, ez), f32),
            vmem((2, 8, 64, 2 * ez), f32),
            vmem((groups, 2 * ez, lanes), bf),
            vmem((groups, 512, lanes), bf),
            vmem((groups, 2 * ez, lanes), bf),
            vmem((512, 2 * ez), f32),
            vmem((3, n, 1, cap), f32),
            vmem((3, n, 1, cap), f32),
            vmem((3, 2, 2, 64, ez), f32),
            vmem((3, 2, 2, 8, 8, ez), f32),
            vmem((3, 4, 2, 8, ez), f32),
            pltpu.SemaphoreType.DMA((3,)),
            pltpu.SemaphoreType.DMA((3,)),
            pltpu.SemaphoreType.DMA((3, 8)),
            pltpu.SemaphoreType.DMA((3, 8)),
        ],
        compiler_params=pltpu.CompilerParams(collective_id=0, has_side_effects=True),
        name="advance",
    )(
        scalar.reshape(2, 8, 64, ez), velocity.reshape(3, 2, 8, 64, ez), diffusivity.reshape(2, ez),
        wm, step_mass, ops, basis, donor, slot_q, slot_e,
    )
    return out.reshape(scalar.shape)


def solution(mesh):
    return jax.shard_map(
        body,
        mesh=mesh,
        in_specs=(
            P(None, None, "gx", "gy", None),
            P(None, None, None, "gx", "gy", None),
            P(None, "gx", "gy", None),
            P(("gx", "gy"), None),
            P(("gx", "gy")),
            P(("gx", "gy")),
            P(None, ("gx", "gy")),
        ),
        out_specs=P(None, None, "gx", "gy", None),
        check_vma=False,
    )
```

```python
import functools
import jax
import jax.numpy as jnp
import numpy as np
from jax import lax
from jax.experimental import pallas as pl
from jax.experimental.pallas import tpu as pltpu
from jax.sharding import PartitionSpec as P

time_step = 0.01
penalty_rate = 50.0
metric = 2.0
volume_factor = 0.125
node_inner = [0.8717401485096066, 0.5917001814331423, 0.20929921790247888]


def legendre_seven(point):
    before, current = (1.0, point)
    for order in range(1, 7):
        before, current = (
            current,
            ((2 * order + 1) * point * current - order * before) / (order + 1),
        )
    return current


def gll_tables():
    degree = 7
    gll_nodes = [
        -1.0,
        -node_inner[0],
        -node_inner[1],
        -node_inner[2],
        node_inner[2],
        node_inner[1],
        node_inner[0],
        1.0,
    ]
    end_values = [legendre_seven(v) for v in gll_nodes]
    weights = [2.0 / (degree * (degree + 1) * v * v) for v in end_values]
    derivative = [[0.0] * 8 for _ in range(8)]
    for a in range(8):
        for b in range(8):
            if a != b:
                derivative[a][b] = end_values[a] / (end_values[b] * (gll_nodes[a] - gll_nodes[b]))
    derivative[0][0] = -degree * (degree + 1) / 4.0
    derivative[7][7] = degree * (degree + 1) / 4.0
    weight_row = jnp.asarray(weights, jnp.float32)
    cube_weights = weight_row[:, None, None] * weight_row[None, :, None] * weight_row[None, None, :]
    return (gll_nodes, cube_weights, derivative)


MESH = pl.DeviceIdType.MESH
HEADINGS = [(-1, 0), (1, 0), (0, -1), (0, 1), (-1, -1), (-1, 1), (1, -1), (1, 1)]


def halves(value):
    high = value.astype(jnp.bfloat16)
    return high, (value - high.astype(jnp.float32)).astype(jnp.bfloat16)


def mm(a, b):
    return jnp.dot(a, b, preferred_element_type=jnp.float32)


def mm_t(a, b):
    return lax.dot_general(a, b, (((1,), (1,)), ((), ())), preferred_element_type=jnp.float32)


def mm3(op_high, op_low, value):
    high, low = halves(value)
    return mm(op_high, high) + mm(op_high, low) + mm(op_low, high)


def step_kernel(
    derivative, gll_nodes, start_ref, vel_ref, nu_ref, wm_ref, dim_ref, ops_ref, asked_ref, slot_q_ref, slot_e_ref,
    out_ref,
    cur, local, work, grad, pick, spread_q, spread_e, count, ans, rep, hx, hy, he, got, basis_ref,
    ask_send, ask_recv,
    ans_send, ans_recv, halo_send, halo_recv,
):
    gx, gy = lax.axis_index("gx"), lax.axis_index("gy")
    nx, ny = lax.axis_size("gx"), lax.axis_size("gy")
    n = nx * ny
    me = gx * ny + gy
    ez = start_ref.shape[-1]
    groups, _, lanes = slot_q_ref.shape
    cap = ans.shape[-1]
    per = lanes // cap

    barrier = pltpu.get_barrier_semaphore()

    def greet(step, carry):
        d = lax.rem(me + step, n)
        pl.semaphore_signal(barrier, inc=1, device_id=(d // ny, lax.rem(d, ny)), device_id_type=MESH)
        return carry

    hx[...] = jnp.zeros_like(hx)
    hy[...] = jnp.zeros_like(hy)
    he[...] = jnp.zeros_like(he)
    lax.fori_loop(1, n, greet, 0)

    pl.semaphore_wait(barrier, n - 1)

    def ask(step, carry):
        d = lax.rem(me + step, n)
        pltpu.make_async_remote_copy(
            src_ref=asked_ref.at[d], dst_ref=got.at[me], send_sem=ask_send, recv_sem=ask_recv,
            device_id=(d // ny, lax.rem(d, ny)), device_id_type=MESH,
        ).start()
        return carry

    lax.fori_loop(1, n, ask, 0)
    count[...] = jnp.zeros_like(count)

    def build(g, carry):
        wide = lax.broadcasted_iota(jnp.int32, (2 * ez, lanes), 0)
        tall = lax.broadcasted_iota(jnp.int32, (512, lanes), 0)
        spread_e[g] = jnp.where(wide == slot_e_ref[g], 1.0, 0.0).astype(jnp.bfloat16)
        spread_q[g] = jnp.where(tall == slot_q_ref[g], 1.0, 0.0).astype(jnp.bfloat16)
        count[...] += mm_t(spread_q[g], spread_e[g])
        return carry

    lax.fori_loop(0, groups, build, 0)
    cur[...] = start_ref[...]
    got[me] = asked_ref[me]
    first = got.at[pl.ds(0, n - 1)]
    pltpu.make_async_copy(first, first, ask_recv).wait()

    def prepare(g, carry):
        asked = jnp.concatenate([got[g * per + t] for t in range(per)], axis=1)
        wide = lax.broadcasted_iota(jnp.int32, (2 * ez, lanes), 0)
        pick[g] = jnp.where(wide == asked[3:4].astype(jnp.int32), 1.0, 0.0).astype(jnp.bfloat16)
        for j in range(8):
            factor = jnp.ones_like(asked)
            for k in range(8):
                if k != j:
                    factor = factor * ((asked - gll_nodes[k]) * (1.0 / (gll_nodes[j] - gll_nodes[k])))
            for c in range(3):
                basis_ref[g, 8 * c + j:8 * c + j + 1, :] = factor[c:c + 1]
        return carry

    lax.fori_loop(0, groups, prepare, 0)

    def halo_copy(s, number):
        dx, dy = HEADINGS[number]
        rows = pl.ds(0 if dy < 0 else 56, 8)
        plane = 0 if dx < 0 else 7
        if dy == 0:
            source, target = local.at[:, plane], hx.at[s, number]
        elif dx == 0:
            source, target = local.at[:, :, rows, :], hy.at[s, number - 2]
        else:
            source, target = local.at[:, plane, rows, :], he.at[s, number - 4]
        return pltpu.make_async_remote_copy(
            src_ref=source, dst_ref=target, send_sem=halo_send.at[s, number], recv_sem=halo_recv.at[s, number],
            device_id=(gx + dx, gy + dy), device_id_type=MESH,
        )

    def inside(dx, dy):
        return (gx + dx >= 0) & (gx + dx < nx) & (gy + dy >= 0) & (gy + dy < ny)

    for s in range(3):
        both = jnp.concatenate([cur[0].reshape(512, ez), cur[1].reshape(512, ez)], axis=1)
        high, low = halves(both)

        def interpolate(g, carry):
            found = mm(high, pick[g]) + mm(low, pick[g])
            acc = found[0:64] * basis_ref[g, 0:1, :]
            for i in range(1, 8):
                acc = acc + found[64 * i:64 * i + 64] * basis_ref[g, i:i + 1, :]
            acc2 = acc[0:8] * basis_ref[g, 8:9, :]
            for j in range(1, 8):
                acc2 = acc2 + acc[8 * j:8 * j + 8] * basis_ref[g, 8 + j:9 + j, :]
            row = jnp.sum(acc2 * basis_ref[g, 16:24, :], axis=0, keepdims=True)
            for t in range(per):
                ans[s, g * per + t] = row[:, t * cap:(t + 1) * cap]
            return carry

        lax.fori_loop(0, groups, interpolate, 0)

        def send(step, carry):
            d = lax.rem(me + step, n)
            pltpu.make_async_remote_copy(
                src_ref=ans.at[s, d], dst_ref=rep.at[s, me], send_sem=ans_send.at[s], recv_sem=ans_recv.at[s],
                device_id=(d // ny, lax.rem(d, ny)), device_id_type=MESH,
            ).start()
            return carry

        lax.fori_loop(1, n, send, 0)

        for m in range(2):
            lo_lane = m * ez
            scale = nu_ref[m:m + 1, :]
            for half in range(2):
                part = cur[m, 4 * half:4 * half + 4].reshape(256, ez)
                grad[0, 4 * half:4 * half + 4, :, lo_lane:lo_lane + ez] = mm3(ops_ref[0], ops_ref[1], part).reshape(4, 64, ez)
                grad[1, 4 * half:4 * half + 4, :, lo_lane:lo_lane + ez] = mm3(ops_ref[2], ops_ref[3], part).reshape(4, 64, ez)
            for a in range(8):
                gxa = (2.0 * derivative[a][0]) * cur[m, 0]
                for i in range(1, 8):
                    gxa = gxa + (2.0 * derivative[a][i]) * cur[m, i]
                wm = wm_ref[a]
                gya = grad[0, a, :, lo_lane:lo_lane + ez]
                gza = grad[1, a, :, lo_lane:lo_lane + ez]
                adv = vel_ref[0, m, a] * gxa + vel_ref[1, m, a] * gya + vel_ref[2, m, a] * gza
                local[m, a] = -(wm * adv)
                wn = wm * scale
                work[m, a] = wn * gxa
                grad[0, a, :, lo_lane:lo_lane + ez] = wn * gya
                grad[1, a, :, lo_lane:lo_lane + ez] = wn * gza
            for half in range(2):
                part_y = grad[0, 4 * half:4 * half + 4, :, lo_lane:lo_lane + ez].reshape(256, ez)
                part_z = grad[1, 4 * half:4 * half + 4, :, lo_lane:lo_lane + ez].reshape(256, ez)
                back = mm3(ops_ref[4], ops_ref[5], part_y) + mm3(ops_ref[6], ops_ref[7], part_z)
                local[m, 4 * half:4 * half + 4] -= back.reshape(4, 64, ez)
            for i in range(8):
                total = (2.0 * derivative[0][i]) * work[m, 0]
                for a in range(1, 8):
                    total = total + (2.0 * derivative[a][i]) * work[m, a]
                local[m, i] -= total

        rep[s, me] = ans[s, me]
        whole = rep.at[s, pl.ds(0, n - 1)]
        pltpu.make_async_copy(whole, whole, ans_recv.at[s]).wait()

        work[...] = jnp.zeros_like(work)

        def scatter(g, carry):
            row = jnp.concatenate([rep[s, g * per + t] for t in range(per)], axis=1)
            row_high, row_low = halves(row)
            where_e = spread_e[g]
            added = mm_t(spread_q[g], where_e * row_high) + mm_t(spread_q[g], where_e * row_low)
            work[0] += added[:, :ez].reshape(8, 64, ez)
            work[1] += added[:, ez:].reshape(8, 64, ez)
            return carry

        lax.fori_loop(0, groups, scatter, 0)
        for m in range(2):
            for i in range(8):
                held = count[64 * i:64 * i + 64, m * ez:(m + 1) * ez]
                local[m, i] += penalty_rate * wm_ref[i] * (work[m, i] - held * cur[m, i])

        for number, (dx, dy) in enumerate(HEADINGS):
            @pl.when(inside(dx, dy))
            def _(number=number):
                halo_copy(s, number).start()

        for number, (dx, dy) in enumerate(HEADINGS):
            @pl.when(inside(-dx, -dy))
            def _(number=number):
                halo_copy(s, number).wait_recv()

        work[...] = local[...]
        for m in range(2):
            work[m, 7] += hx[s, 0, m]
            work[m, 0] += hx[s, 1, m]
            work[m, :, 56:64, :] += hy[s, 0, m]
            work[m, :, 0:8, :] += hy[s, 1, m]
            work[m, 7, 56:64, :] += he[s, 0, m]
            work[m, 7, 0:8, :] += he[s, 1, m]
            work[m, 0, 56:64, :] += he[s, 2, m]
            work[m, 0, 0:8, :] += he[s, 3, m]

        for m in range(2):
            flat = work[m].reshape(512, ez)
            depth = lax.rem(lax.broadcasted_iota(jnp.int32, (512, ez), 0), 8)
            lane = lax.broadcasted_iota(jnp.int32, (512, ez), 1)
            after = pltpu.roll(pltpu.roll(flat, 7, 0), ez - 1, 1)
            before = pltpu.roll(pltpu.roll(flat, 505, 0), 1, 1)
            flat = flat + jnp.where((depth == 7) & (lane < ez - 1), after, 0.0)
            flat = flat + jnp.where((depth == 0) & (lane > 0), before, 0.0)
            moved = cur[m] + flat.reshape(8, 64, ez) * dim_ref[...]
            if s == 0:
                cur[m] = moved
            elif s == 1:
                cur[m] = 0.75 * start_ref[m] + 0.25 * moved
            else:
                out_ref[m] = 2.0 / 3.0 * moved

        for number, (dx, dy) in enumerate(HEADINGS):
            @pl.when(inside(dx, dy))
            def _(number=number):
                halo_copy(s, number).wait_send()

    sent = got.at[pl.ds(0, n - 1)]
    pltpu.make_async_copy(sent, sent, ask_send).wait()
    for s in range(3):
        whole = ans.at[s, pl.ds(0, n - 1)]
        pltpu.make_async_copy(whole, whole, ans_send.at[s]).wait()


def split_host(matrix):
    high = matrix.astype(jnp.bfloat16)
    low = (matrix - high.astype(np.float64)).astype(jnp.bfloat16)
    return [high, low]


def body(scalar, velocity, diffusivity, recv_owner, donor_elem, recv_point, recv_coords):
    gll_nodes, cube_weights, derivative = gll_tables()
    ez = scalar.shape[4]
    elems = scalar.shape[2] * scalar.shape[3] * ez
    width_x, width_y = lax.axis_size("gx"), lax.axis_size("gy")
    n = width_x * width_y
    rows = recv_owner.shape[0]
    cap = max(2, 2 * rows // n)
    slots_all = n * cap
    per = max(1, min(n, 512 // cap))
    groups, lanes = n // per, per * cap

    owners = recv_owner[:, 0]
    bf, f32 = jnp.bfloat16, jnp.float32
    hot = (owners[None, :] == jnp.arange(n, dtype=jnp.int32)[:, None]).astype(bf)
    width = min(256, rows)
    blocks = rows // width
    earlier = jnp.asarray(np.triu(np.ones((width, width)), 1), bf)
    hot3 = hot.reshape(n, blocks, width)
    within = jnp.einsum("nbr,rs->nbs", hot3, earlier, preferred_element_type=f32)
    sums = jnp.sum(hot3.astype(f32), axis=2)
    strict = np.triu(np.ones((blocks, blocks)), 1).astype(np.float32)
    offset = jnp.sum(sums[:, :, None] * strict[None], axis=1)
    rank = jnp.sum((within + offset[:, :, None]) * hot3.astype(f32), axis=0).reshape(rows)
    slot_hot = (rank[None, :].astype(jnp.int32) == jnp.arange(cap, dtype=jnp.int32)[:, None]).astype(bf)

    own_mesh = (jnp.arange(rows, dtype=jnp.int32) >= rows // 2).astype(jnp.int32)
    point_q, point_e = recv_point // elems, recv_point % elems
    high = lax.reduce_precision(recv_coords, 8, 7)
    middle = lax.reduce_precision(recv_coords - high, 8, 7)
    low = recv_coords - high - middle
    ints = jnp.stack([donor_elem, 1 - own_mesh, point_q // 8 + 1, point_q % 8, point_e, own_mesh]).astype(f32)
    data = jnp.concatenate([high, middle, low, ints], axis=0).astype(bf)
    routed = jnp.einsum("cnr,kr->nck", data[:, None, :] * hot[None], slot_hot, preferred_element_type=f32)
    coords = routed[:, 0:3] + routed[:, 3:6] + routed[:, 6:9]
    asked = jnp.concatenate([coords, routed[:, 9:10] + elems * routed[:, 10:11]], axis=1)
    def grouped(piece):
        return piece.astype(jnp.int32).reshape(groups, 1, lanes)

    slot_q = grouped((routed[:, 11] - 1.0) * 8.0 + routed[:, 12])
    slot_e = grouped(routed[:, 13] + elems * routed[:, 14])
    half_eye = np.eye(4)
    table = 2.0 * np.asarray(derivative, np.float64)
    along_y = np.kron(half_eye, np.kron(table, np.eye(8)))
    along_z = np.kron(half_eye, np.kron(np.eye(8), table))
    ops = []
    for matrix in (along_y, along_z, along_y.T, along_z.T):
        ops = ops + split_host(matrix)
    ops = jnp.asarray(np.stack(ops))

    weights = np.asarray([2.0 / (56.0 * legendre_seven(v) ** 2) for v in gll_nodes], np.float64)
    shared = jnp.asarray(weights + weights[::-1] * (np.arange(8) % 7 == 0), f32)
    single = jnp.asarray(weights, f32)
    ends = jnp.arange(8)

    def line_mass(position, count):
        joined = ((ends == 0) & (position > 0)) | ((ends == 7) & (position < count - 1))
        return jnp.where(joined, shared, single)

    mass_x = line_mass(lax.axis_index("gx"), width_x)
    mass_y = line_mass(lax.axis_index("gy"), width_y)
    place = jnp.arange(ez)[None, :]
    joined_z = ((ends[:, None] == 0) & (place > 0)) | ((ends[:, None] == 7) & (place < ez - 1))
    mass_z = jnp.where(joined_z, shared[:, None], single[:, None])
    mass = volume_factor * mass_x[:, None, None, None] * mass_y[None, :, None, None] * mass_z[None, None]
    step_mass = (time_step / mass).reshape(8, 64, ez)
    wm = jnp.broadcast_to((volume_factor * cube_weights).reshape(8, 64, 1), (8, 64, ez))

    vmem = pltpu.VMEM
    out = pl.pallas_call(
        functools.partial(step_kernel, derivative, gll_nodes),
        out_shape=jax.ShapeDtypeStruct((2, 8, 64, ez), f32),
        in_specs=[pl.BlockSpec(memory_space=vmem)] * 9,
        out_specs=pl.BlockSpec(memory_space=vmem),
        scratch_shapes=[
            vmem((2, 8, 64, ez), f32),
            vmem((2, 8, 64, ez), f32),
            vmem((2, 8, 64, ez), f32),
            vmem((2, 8, 64, 2 * ez), f32),
            vmem((groups, 2 * ez, lanes), bf),
            vmem((groups, 512, lanes), bf),
            vmem((groups, 2 * ez, lanes), bf),
            vmem((512, 2 * ez), f32),
            vmem((3, n, 1, cap), f32),
            vmem((3, n, 1, cap), f32),
            vmem((3, 2, 2, 64, ez), f32),
            vmem((3, 2, 2, 8, 8, ez), f32),
            vmem((3, 4, 2, 8, ez), f32),
            vmem((n, 4, cap), f32),
            vmem((groups, 24, lanes), f32),
            pltpu.SemaphoreType.DMA,
            pltpu.SemaphoreType.DMA,
            pltpu.SemaphoreType.DMA((3,)),
            pltpu.SemaphoreType.DMA((3,)),
            pltpu.SemaphoreType.DMA((3, 8)),
            pltpu.SemaphoreType.DMA((3, 8)),
        ],
        compiler_params=pltpu.CompilerParams(collective_id=0, has_side_effects=True),
        name="advance",
    )(
        scalar.reshape(2, 8, 64, ez), velocity.reshape(3, 2, 8, 64, ez), diffusivity.reshape(2, ez),
        wm, step_mass, ops, asked, slot_q, slot_e,
    )
    return scalar / 3.0 + out.reshape(scalar.shape)


def solution(mesh):
    return jax.shard_map(
        body,
        mesh=mesh,
        in_specs=(
            P(None, None, "gx", "gy", None),
            P(None, None, None, "gx", "gy", None),
            P(None, "gx", "gy", None),
            P(("gx", "gy"), None),
            P(("gx", "gy")),
            P(("gx", "gy")),
            P(None, ("gx", "gy")),
        ),
        out_specs=P(None, None, "gx", "gy", None),
        check_vma=False,
    )
```
